32 devices in a mesh: dp: 1 (over z), fsdp: 32 (over y, x, core).
Axes of the slice: x: 4, y: 4, z: 1, core: 2. Of those that a mesh axis runs over, the one named last changes fastest.
The devices are a block of a 4x4x8 slice.
Arguments:
- prompts: bfloat16 [512, 128, 2560], P(('dp', 'fsdp'))
- ln1_gain: bfloat16 [2560], P('fsdp')
- ln1_bias: bfloat16 [2560], P('fsdp')
- w_qkv: bfloat16 [2560, 3, 32, 80], P('fsdp')
- b_qkv: bfloat16 [7680], P('fsdp')
- w_out: bfloat16 [2560, 2560], P('fsdp')
- b_out: bfloat16 [2560], P('fsdp')
- ln2_gain: bfloat16 [2560], P('fsdp')
- ln2_bias: bfloat16 [2560], P('fsdp')
- w_up: bfloat16 [2560, 10240], P('fsdp')
- b_up: bfloat16 [10240], P('fsdp')
- w_down: bfloat16 [10240, 2560], P('fsdp')
- b_down: bfloat16 [2560], P('fsdp')
Outputs:
- output 1: bfloat16 [512, 128, 2560], P(('dp', 'fsdp'))
- output 2: bfloat16 [512, 128, 32, 80], P(('dp', 'fsdp'))
- output 3: bfloat16 [512, 128, 32, 80], P(('dp', 'fsdp'))
All inputs are finite; a program needn't handle non-finite values.
Results may differ from the reference program's by a relative error of at most 0.00904977.
Values are sent between devices in bfloat16 or wider.
A program may use at most 768 MiB of HBM per device.

```python
import jax
import jax.numpy as jnp
from jax import lax

D = 2560
HEADS = 32
HEAD = 80
SEQ = 128
BATCH = 512
FFN = 4 * D
QBLOCK = min(SEQ, 256)
LN_EPS = 1e-5


def draw_normal(key, shape, scale, offset=0.0):
    return (offset + scale * jax.random.normal(key, shape, jnp.float32)).astype(jnp.bfloat16)


def setup_inputs(seed: int = 0, part: int = 0) -> dict:
    keys = jax.random.split(jax.random.key(seed), 13)
    return {
        'prompts': draw_normal(jax.random.fold_in(keys[0], part), (BATCH, SEQ, D), 1.0),
        'ln1_gain': draw_normal(keys[1], (D,), 0.3, 1.0),
        'ln1_bias': draw_normal(keys[2], (D,), 0.3),
        'w_qkv': draw_normal(keys[3], (D, 3, HEADS, HEAD), D ** -0.5),
        'b_qkv': draw_normal(keys[4], (3 * HEADS * HEAD,), 0.5),
        'w_out': draw_normal(keys[5], (HEADS * HEAD, D), (HEADS * HEAD) ** -0.5),
        'b_out': draw_normal(keys[6], (D,), 0.5),
        'ln2_gain': draw_normal(keys[7], (D,), 0.3, 1.0),
        'ln2_bias': draw_normal(keys[8], (D,), 0.3),
        'w_up': draw_normal(keys[9], (D, FFN), D ** -0.5),
        'b_up': draw_normal(keys[10], (FFN,), 0.5),
        'w_down': draw_normal(keys[11], (FFN, D), 1.5 * FFN ** -0.5),
        'b_down': draw_normal(keys[12], (D,), 0.5),
    }


def layer_norm(act, gain, shift):
    act_f32 = act.astype(jnp.float32)
    mean_val = jnp.mean(act_f32, axis=-1, keepdims=True)
    centered = act_f32 - mean_val
    var_val = jnp.mean(centered * centered, axis=-1, keepdims=True)
    normed = centered * lax.rsqrt(var_val + LN_EPS)
    return (normed * gain.astype(jnp.float32) + shift.astype(jnp.float32)).astype(jnp.bfloat16)


def reference(prompts, ln1_gain, ln1_bias, w_qkv, b_qkv, w_out, b_out, ln2_gain, ln2_bias, w_up, b_up, w_down, b_down):
    w_qkv_flat = w_qkv.reshape(D, 3 * HEADS * HEAD)
    key_pos = jnp.arange(SEQ)

    def one_prompt(prompt):
        normed1 = layer_norm(prompt, ln1_gain, ln1_bias)
        proj_qkv = jnp.dot(normed1, w_qkv_flat, preferred_element_type=jnp.float32)
        proj_qkv = (proj_qkv + b_qkv.astype(jnp.float32)).astype(jnp.bfloat16).reshape(SEQ, 3, HEADS, HEAD)
        keys_f32 = proj_qkv[:, 1].astype(jnp.float32)
        values_f32 = proj_qkv[:, 2].astype(jnp.float32)
        query_blocks = proj_qkv[:, 0].astype(jnp.float32).reshape(SEQ // QBLOCK, QBLOCK, HEADS, HEAD)

        def one_block(block_in):
            q_blk, blk_idx = block_in
            scores = jnp.einsum('qhe,khe->hqk', q_blk, keys_f32) * (HEAD ** -0.5)
            query_pos = blk_idx * QBLOCK + jnp.arange(QBLOCK)
            allowed = key_pos[None, :] <= query_pos[:, None]
            scores = jnp.where(allowed[None], scores, -jnp.inf)
            probs = jax.nn.softmax(scores, axis=-1).astype(jnp.bfloat16)
            context = jnp.einsum('hqk,khe->qhe', probs.astype(jnp.float32), values_f32)
            return context.astype(jnp.bfloat16)

        context = lax.map(one_block, (query_blocks, jnp.arange(SEQ // QBLOCK))).reshape(SEQ, HEADS * HEAD)
        attn_out = jnp.dot(context, w_out, preferred_element_type=jnp.float32)
        resid = (prompt.astype(jnp.float32) + attn_out + b_out.astype(jnp.float32)).astype(jnp.bfloat16)
        normed2 = layer_norm(resid, ln2_gain, ln2_bias)
        hidden = jnp.dot(normed2, w_up, preferred_element_type=jnp.float32) + b_up.astype(jnp.float32)
        hidden = jax.nn.gelu(hidden, approximate=True).astype(jnp.bfloat16)
        mlp_out = jnp.dot(hidden, w_down, preferred_element_type=jnp.float32)
        out_one = (resid.astype(jnp.float32) + mlp_out + b_down.astype(jnp.float32)).astype(jnp.bfloat16)
        return out_one, proj_qkv[:, 1], proj_qkv[:, 2]

    layer_out, k_cache, v_cache = lax.map(one_prompt, prompts)
    return layer_out, k_cache, v_cache
```

```python
import functools

import jax
import jax.numpy as jnp
from jax import lax
from jax.experimental import pallas as pl
from jax.experimental.pallas import tpu as pltpu
from jax.sharding import PartitionSpec as P

LN_EPS = 1e-5
LANES = 128
F32 = jnp.float32
BF16 = jnp.bfloat16


def layer_norm(act, gain, shift):
    act_f32 = act.astype(F32)
    mean_val = jnp.mean(act_f32, axis=-1, keepdims=True)
    centered = act_f32 - mean_val
    var_val = jnp.mean(centered * centered, axis=-1, keepdims=True)
    normed = centered * lax.rsqrt(var_val + LN_EPS)
    return (normed * gain + shift).astype(BF16)


def params(limit_mib, axes):
    return pltpu.CompilerParams(
        dimension_semantics=("arbitrary",) * axes, vmem_limit_bytes=limit_mib << 20
    )


def cost(flops, nbytes):
    return pl.CostEstimate(flops=int(flops), bytes_accessed=int(nbytes), transcendentals=0)


def row_chunks(rows, size):
    return [(start, min(size, rows - start)) for start in range(0, rows, size)]


def proj_kernel(epilogue, chunk, x_ref, w_ref, b_ref, o_ref):
    for start, size in row_chunks(x_ref.shape[0], chunk):
        acc = jnp.dot(x_ref[start:start + size, :], w_ref[...], preferred_element_type=F32)
        o_ref[start:start + size, :] = epilogue(acc + b_ref[...]).astype(o_ref.dtype)


def project(x, w, first_col, n_cols, bias, epilogue, bm, bn, chunk=256):
    rows, k = x.shape
    off = first_col // bn
    return pl.pallas_call(
        functools.partial(proj_kernel, epilogue, chunk),
        out_shape=jax.ShapeDtypeStruct((rows, n_cols), BF16),
        grid=(rows // bm, n_cols // bn),
        in_specs=[
            pl.BlockSpec((bm, k), lambda m, n: (m, 0)),
            pl.BlockSpec((k, bn), lambda m, n: (0, n + off)),
            pl.BlockSpec((1, bn), lambda m, n: (0, n)),
        ],
        out_specs=pl.BlockSpec((bm, bn), lambda m, n: (m, n)),
        compiler_params=params(58, 2),
        cost_estimate=cost(2 * rows * k * n_cols, 2 * (rows * k + k * n_cols + rows * n_cols)),
    )(x, w, bias)


def kv_kernel(half, bn, seq, chunk, x_ref, w_ref, b_ref, k_hbm, v_hbm, buf, sem):
    n = pl.program_id(0)
    total = 2 * half
    slot = lax.rem(n, 2)

    def copy(dst, col_block, which):
        cols = pl.ds(pl.multiple_of(col_block * bn, bn), bn)
        return pltpu.make_async_copy(buf.at[which], dst.at[:, cols, :], sem.at[which])

    @pl.when(n >= 2)
    def _():
        copy(k_hbm, 0, slot).wait()

    for start, size in row_chunks(x_ref.shape[0], chunk):
        acc = jnp.dot(x_ref[start:start + size, :], w_ref[...], preferred_element_type=F32)
        turned = (acc + b_ref[...]).astype(BF16).T
        for i in range(size // seq):
            buf[slot, start // seq + i] = turned[:, i * seq:(i + 1) * seq]

    @pl.when(n < half)
    def _():
        copy(k_hbm, n, slot).start()

    @pl.when(n >= half)
    def _():
        copy(v_hbm, n - half, slot).start()

    @pl.when(n == total - 1)
    def _():
        copy(v_hbm, 0, 1 - slot).wait()
        copy(v_hbm, 0, slot).wait()


def keys_values(x, w, first_col, width, bias, seq, bn=256, chunk=256):
    rows, k = x.shape
    batch = rows // seq
    off, half = first_col // bn, width // bn
    shape = jax.ShapeDtypeStruct((batch, width, seq), BF16)
    return pl.pallas_call(
        functools.partial(kv_kernel, half, bn, seq, chunk),
        out_shape=(shape, shape),
        grid=(2 * half,),
        in_specs=[
            pl.BlockSpec((rows, k), lambda n: (0, 0), pipeline_mode=pl.Buffered(1)),
            pl.BlockSpec((k, bn), lambda n: (0, n + off)),
            pl.BlockSpec((1, bn), lambda n: (0, n)),
        ],
        out_specs=(pl.BlockSpec(memory_space=pl.ANY), pl.BlockSpec(memory_space=pl.ANY)),
        scratch_shapes=[pltpu.VMEM((2, batch, bn, seq), BF16), pltpu.SemaphoreType.DMA((2,))],
        compiler_params=params(58, 1),
        cost_estimate=cost(4 * rows * k * width, 2 * (rows * k + 2 * k * width + 2 * rows * width)),
    )(x, w, bias)


def attn_kernel(heads, head_dim, q_ref, k_ref, v_ref, o_ref):
    seq = q_ref.shape[0]
    scale = head_dim ** -0.5
    query = lax.broadcasted_iota(jnp.int32, (seq, seq), 0)
    key = lax.broadcasted_iota(jnp.int32, (seq, seq), 1)
    allowed = key <= query
    columns = {}
    for h in range(heads):
        lo, hi = h * head_dim, (h + 1) * head_dim
        base = lo // LANES * LANES
        width = pl.cdiv(hi - base, LANES) * LANES

        def padded(ref):
            parts = [ref[0, lo:hi, :]]
            if lo > base:
                parts.insert(0, jnp.zeros((lo - base, seq), BF16))
            if base + width > hi:
                parts.append(jnp.zeros((base + width - hi, seq), BF16))
            return jnp.concatenate(parts, axis=0) if len(parts) > 1 else parts[0]

        scores = jnp.dot(q_ref[:, base:base + width], padded(k_ref), preferred_element_type=F32) * scale
        scores = jnp.where(allowed, scores, -jnp.inf)
        peak = jnp.max(scores, axis=-1, keepdims=True)
        weights = jnp.exp(scores - peak)
        probs = (weights * (1.0 / jnp.sum(weights, axis=-1, keepdims=True))).astype(BF16)
        part = lax.dot_general(probs, padded(v_ref), (((1,), (1,)), ((), ())), preferred_element_type=F32)
        for i in range(width // LANES):
            col = base // LANES + i
            piece = part[:, i * LANES:(i + 1) * LANES]
            columns[col] = columns[col] + piece if col in columns else piece
        for col in [c for c in columns if (c + 1) * LANES <= hi]:
            o_ref[:, col * LANES:(col + 1) * LANES] = columns.pop(col).astype(BF16)


def attention(q, k_t, v_t, heads, head_dim):
    batch, width, seq = k_t.shape
    side = pl.BlockSpec((1, width, seq), lambda b: (b, 0, 0))
    flat = pl.BlockSpec((seq, width), lambda b: (b, 0))
    return pl.pallas_call(
        functools.partial(attn_kernel, heads, head_dim),
        out_shape=jax.ShapeDtypeStruct((batch * seq, width), BF16),
        grid=(batch,),
        in_specs=[flat, side, side],
        out_specs=flat,
        compiler_params=params(48, 1),
        cost_estimate=cost(12 * batch * heads * seq * seq * LANES, 8 * batch * seq * width),
    )(q, k_t, v_t)


def sum_kernel(n_terms, chunk, *refs):
    xs, ws = refs[:n_terms], refs[n_terms:2 * n_terms]
    base_ref, b_ref, o_ref = refs[2 * n_terms:]
    for start, size in row_chunks(o_ref.shape[0], chunk):
        acc = base_ref[start:start + size, :].astype(F32)
        for x_ref, w_ref in zip(xs, ws):
            acc = acc + jnp.dot(x_ref[start:start + size, :], w_ref[...], preferred_element_type=F32)
        if b_ref is not None:
            acc = acc + b_ref[...]
        o_ref[start:start + size, :] = acc.astype(o_ref.dtype)


def add_products(terms, base, bias, out_dtype, bm, bn, chunk=256):
    rows, cols = base.shape
    k = terms[0][2].shape[0]
    n_terms = len(terms)
    kernel = functools.partial(sum_kernel, n_terms, chunk)
    specs = [pl.BlockSpec((bm, k), functools.partial(lambda o, m, n: (m, o), xc // k)) for _, xc, _, _ in terms]
    specs += [pl.BlockSpec((k, bn), functools.partial(lambda o, m, n: (0, n + o), wc // bn)) for _, _, _, wc in terms]
    specs.append(pl.BlockSpec((bm, bn), lambda m, n: (m, n)))
    args = [t[0] for t in terms] + [t[2] for t in terms] + [base]
    if bias is not None:
        specs.append(pl.BlockSpec((1, bn), lambda m, n: (0, n)))
        args.append(bias)
        body = kernel
    else:
        def body(*refs):
            kernel(*refs[:-1], None, refs[-1])
    return pl.pallas_call(
        body,
        out_shape=jax.ShapeDtypeStruct((rows, cols), out_dtype),
        grid=(rows // bm, cols // bn),
        in_specs=specs,
        out_specs=pl.BlockSpec((bm, bn), lambda m, n: (m, n)),
        compiler_params=params(58, 2),
        cost_estimate=cost(2 * n_terms * rows * k * cols, 2 * n_terms * (rows * k + k * cols) + 6 * rows * cols),
    )(*args)


def solution(mesh):
    batch_axes = ('dp', 'fsdp')
    n_dev = mesh.shape['fsdp']

    def gather_full(shard):
        return lax.all_gather(shard, 'fsdp', axis=0, tiled=True)

    def local_layer(prompts, ln1_gain, ln1_bias, w_qkv, b_qkv, w_out, b_out, ln2_gain, ln2_bias, w_up, b_up, w_down, b_down):
        batch, seq, d = prompts.shape
        heads, head_dim = w_qkv.shape[2], w_qkv.shape[3]
        width = heads * head_dim
        own = w_out.shape[0]
        n_slabs = w_up.shape[1] // d
        rows = batch * seq

        small = jnp.concatenate(
            [v.reshape(-1, own) for v in (ln1_gain, ln1_bias, b_out, ln2_gain, ln2_bias, b_down, b_qkv, b_up)], axis=0)
        n_small = small.shape[0]
        small = jnp.pad(small, ((0, -n_small % 16), (0, -own % LANES)))
        up_slabs = w_up.reshape(own, n_dev, n_slabs, own).transpose(0, 2, 1, 3).reshape(own, n_slabs * d)
        down_slabs = [w_down[u * own:(u + 1) * own] for u in range(n_slabs)]

        cut = (n_slabs - 1) * d
        full_a = gather_full(w_qkv.reshape(own, 3 * width))
        vectors = lax.all_gather(small, 'fsdp', axis=0, tiled=False)[:, :n_small, :own].astype(F32)
        full_b = gather_full(jnp.concatenate([w_out, up_slabs[:, :cut]], axis=1))
        full_c = gather_full(jnp.concatenate([up_slabs[:, cut:], down_slabs[0], down_slabs[1]], axis=1))
        full_d = gather_full(jnp.concatenate(down_slabs[2:], axis=1))

        bqkv = vectors[:, 6:9].reshape(1, 3 * width)
        vectors = vectors.transpose(1, 0, 2).reshape(n_small, d)
        g1, s1, bo, g2, s2, bd = vectors[0], vectors[1], vectors[2:3], vectors[3], vectors[4], vectors[5:6]
        bup = vectors[9:].reshape(1, n_slabs * d)

        x = prompts.reshape(rows, d)
        normed1 = layer_norm(x, g1, s1)
        identity = lambda t: t
        gelu = functools.partial(jax.nn.gelu, approximate=True)
        k_t, v_t = keys_values(normed1, full_a, width, width, bqkv[:, width:], seq)
        q = project(normed1, full_a, 0, width, bqkv[:, :width], identity, rows // 2, 512)
        ctx = attention(q, k_t, v_t, heads, head_dim)
        x1 = add_products([(ctx, 0, full_b, 0)], x, bo, BF16, rows // 2, 512)
        normed2 = layer_norm(x1, g2, s2)
        hid_a = project(normed2, full_b, width, cut, bup[:, :cut], gelu, rows // 2, 512)
        normed2, hid_a = lax.optimization_barrier((normed2, hid_a))
        hid_b = project(normed2, full_c, 0, d, bup[:, cut:], gelu, rows // 2, 512)
        part = add_products([(hid_a, 0, full_c, d), (hid_a, d, full_c, 2 * d)], x1, bd, F32, rows // 2, 256)
        y = add_products([(hid_a, 2 * d, full_d, 0), (hid_b, 0, full_d, d)], part, None, BF16, rows // 2, 256)

        def cache(t):
            return t.reshape(batch, heads, head_dim, seq).transpose(0, 3, 1, 2)

        return y.reshape(batch, seq, d), cache(k_t), cache(v_t)

    weight_spec = P('fsdp')
    return jax.shard_map(local_layer, mesh=mesh, in_specs=(P(batch_axes),) + (weight_spec,) * 12, out_specs=(P(batch_axes), P(batch_axes), P(batch_axes)), check_vma=False)
```

```python
import functools

import jax
import jax.numpy as jnp
from jax import lax
from jax.experimental import pallas as pl
from jax.experimental.pallas import tpu as pltpu
from jax.sharding import PartitionSpec as P

LN_EPS = 1e-5
LANES = 128
F32 = jnp.float32
BF16 = jnp.bfloat16


def layer_norm(act, gain, shift):
    act_f32 = act.astype(F32)
    mean_val = jnp.mean(act_f32, axis=-1, keepdims=True)
    centered = act_f32 - mean_val
    var_val = jnp.mean(centered * centered, axis=-1, keepdims=True)
    normed = centered * lax.rsqrt(var_val + LN_EPS)
    return (normed * gain + shift).astype(BF16)


def params(limit_mib, axes):
    return pltpu.CompilerParams(
        dimension_semantics=("arbitrary",) * axes, vmem_limit_bytes=limit_mib << 20
    )


def cost(flops, nbytes):
    return pl.CostEstimate(flops=int(flops), bytes_accessed=int(nbytes), transcendentals=0)


def row_chunks(rows, size):
    return [(start, min(size, rows - start)) for start in range(0, rows, size)]


def proj_kernel(epilogue, chunk, x_ref, w_ref, b_ref, o_ref):
    for start, size in row_chunks(x_ref.shape[0], chunk):
        acc = jnp.dot(x_ref[start:start + size, :], w_ref[...], preferred_element_type=F32)
        o_ref[start:start + size, :] = epilogue(acc + b_ref[...]).astype(o_ref.dtype)


def project(x, w, first_col, n_cols, bias, epilogue, bm, bn, chunk=256):
    rows, k = x.shape
    off = first_col // bn
    return pl.pallas_call(
        functools.partial(proj_kernel, epilogue, chunk),
        out_shape=jax.ShapeDtypeStruct((rows, n_cols), BF16),
        grid=(rows // bm, n_cols // bn),
        in_specs=[
            pl.BlockSpec((bm, k), lambda m, n: (m, 0), pipeline_mode=pl.Buffered(1 if bm == rows else 2)),
            pl.BlockSpec((k, bn), lambda m, n: (0, n + off)),
            pl.BlockSpec((1, bn), lambda m, n: (0, n)),
        ],
        out_specs=pl.BlockSpec((bm, bn), lambda m, n: (m, n)),
        compiler_params=params(58, 2),
        cost_estimate=cost(2 * rows * k * n_cols, 2 * (rows * k + k * n_cols + rows * n_cols)),
    )(x, w, bias)


def qkv_kernel(part, bn, seq, chunk, x_ref, w_ref, b_ref, q_hbm, k_hbm, v_hbm, flat, buf, flat_sem, sem):
    n = pl.program_id(0)
    slot = lax.rem(n, 2)

    def flat_copy(block, which):
        cols = pl.ds(pl.multiple_of(block * bn, bn), bn)
        return pltpu.make_async_copy(flat.at[which], q_hbm.at[:, cols], flat_sem.at[which])

    def copy(dst, block, which):
        cols = pl.ds(pl.multiple_of(block * bn, bn), bn)
        return pltpu.make_async_copy(buf.at[which], dst.at[:, cols, :], sem.at[which])

    def product(start, size):
        acc = jnp.dot(x_ref[start:start + size, :], w_ref[...], preferred_element_type=F32)
        return (acc + b_ref[...]).astype(BF16)

    @pl.when((n >= 2) & (n < part + 2))
    def _():
        flat_copy(0, slot).wait()

    @pl.when(n >= part + 2)
    def _():
        copy(k_hbm, 0, slot).wait()

    @pl.when(n < part)
    def _():
        for start, size in row_chunks(x_ref.shape[0], chunk):
            flat[slot, start:start + size, :] = product(start, size)
        flat_copy(n, slot).start()

    @pl.when(n >= part)
    def _():
        for start, size in row_chunks(x_ref.shape[0], chunk):
            turned = product(start, size).T
            for i in range(size // seq):
                buf[slot, start // seq + i] = turned[:, i * seq:(i + 1) * seq]

    @pl.when((n >= part) & (n < 2 * part))
    def _():
        copy(k_hbm, n - part, slot).start()

    @pl.when(n >= 2 * part)
    def _():
        copy(v_hbm, n - 2 * part, slot).start()

    @pl.when(n == 3 * part - 1)
    def _():
        copy(v_hbm, 0, 1 - slot).wait()
        copy(v_hbm, 0, slot).wait()


def queries_keys_values(x, w, width, bias, seq, bn=256, chunk=256):
    rows, k = x.shape
    batch = rows // seq
    part = width // bn
    turned = jax.ShapeDtypeStruct((batch, width, seq), BF16)
    anywhere = pl.BlockSpec(memory_space=pl.ANY)
    return pl.pallas_call(
        functools.partial(qkv_kernel, part, bn, seq, chunk),
        out_shape=(jax.ShapeDtypeStruct((rows, width), BF16), turned, turned),
        grid=(3 * part,),
        in_specs=[
            pl.BlockSpec((rows, k), lambda n: (0, 0), pipeline_mode=pl.Buffered(1)),
            pl.BlockSpec((k, bn), lambda n: (0, n)),
            pl.BlockSpec((1, bn), lambda n: (0, n)),
        ],
        out_specs=(anywhere, anywhere, anywhere),
        scratch_shapes=[
            pltpu.VMEM((2, rows, bn), BF16),
            pltpu.VMEM((2, batch, bn, seq), BF16),
            pltpu.SemaphoreType.DMA((2,)),
            pltpu.SemaphoreType.DMA((2,)),
        ],
        compiler_params=params(58, 1),
        cost_estimate=cost(6 * rows * k * width, 2 * (rows * k + 3 * k * width + 3 * rows * width)),
    )(x, w, bias)


def norm_kernel(chunk, x_ref, g_ref, s_ref, o_ref):
    for start, size in row_chunks(x_ref.shape[0], chunk):
        o_ref[start:start + size, :] = layer_norm(x_ref[start:start + size, :], g_ref[...], s_ref[...])


def norm_rows(x, gain, shift, bm=256, chunk=16):
    rows, d = x.shape
    block = pl.BlockSpec((bm, d), lambda m: (m, 0))
    vector = pl.BlockSpec((1, d), lambda m: (0, 0))
    return pl.pallas_call(
        functools.partial(norm_kernel, chunk),
        out_shape=jax.ShapeDtypeStruct((rows, d), BF16),
        grid=(rows // bm,),
        in_specs=[block, vector, vector],
        out_specs=block,
        compiler_params=params(32, 1),
        cost_estimate=cost(10 * rows * d, 4 * rows * d),
    )(x, gain, shift)


def attn_kernel(heads, head_dim, q_ref, k_ref, v_ref, o_ref):
    seq = q_ref.shape[0]
    scale = head_dim ** -0.5
    query = lax.broadcasted_iota(jnp.int32, (seq, seq), 0)
    key = lax.broadcasted_iota(jnp.int32, (seq, seq), 1)
    allowed = key <= query
    columns = {}
    group = 2
    for first in range(0, heads, group):
        members = [(h * head_dim, (h + 1) * head_dim) for h in range(first, first + group)]
        base = members[0][0] // LANES * LANES
        last = members[-1][1]
        width = pl.cdiv(last - base, LANES) * LANES

        def window(ref, lo, hi):
            parts = [ref[0, lo:hi, :]]
            if lo > base:
                parts.insert(0, jnp.zeros((lo - base, seq), BF16))
            if base + width > hi:
                parts.append(jnp.zeros((base + width - hi, seq), BF16))
            return jnp.concatenate(parts, axis=0) if len(parts) > 1 else parts[0]

        def side_by_side(ref):
            return jnp.concatenate([window(ref, lo, hi) for lo, hi in members], axis=1)

        both = jnp.dot(q_ref[:, base:base + width], side_by_side(k_ref), preferred_element_type=F32)
        probs = []
        for i in range(group):
            scores = jnp.where(allowed, both[:, i * seq:(i + 1) * seq] * scale, -jnp.inf)
            peak = jnp.max(scores, axis=-1, keepdims=True)
            weights = jnp.exp(scores - peak)
            probs.append((weights * (1.0 / jnp.sum(weights, axis=-1, keepdims=True))).astype(BF16))
        part = lax.dot_general(
            jnp.concatenate(probs, axis=1), side_by_side(v_ref), (((1,), (1,)), ((), ())), preferred_element_type=F32)
        for i in range(width // LANES):
            col = base // LANES + i
            piece = part[:, i * LANES:(i + 1) * LANES]
            columns[col] = columns[col] + piece if col in columns else piece
        for col in [c for c in columns if (c + 1) * LANES <= last]:
            o_ref[:, col * LANES:(col + 1) * LANES] = columns.pop(col).astype(BF16)


def attention(q, k_t, v_t, heads, head_dim):
    batch, width, seq = k_t.shape
    side = pl.BlockSpec((1, width, seq), lambda b: (b, 0, 0))
    flat = pl.BlockSpec((seq, width), lambda b: (b, 0))
    return pl.pallas_call(
        functools.partial(attn_kernel, heads, head_dim),
        out_shape=jax.ShapeDtypeStruct((batch * seq, width), BF16),
        grid=(batch,),
        in_specs=[flat, side, side],
        out_specs=flat,
        compiler_params=params(48, 1),
        cost_estimate=cost(12 * batch * heads * seq * seq * LANES, 8 * batch * seq * width),
    )(q, k_t, v_t)


def sum_kernel(n_terms, chunk, *refs):
    xs, ws = refs[:n_terms], refs[n_terms:2 * n_terms]
    base_ref, b_ref, o_ref = refs[2 * n_terms:]
    for start, size in row_chunks(o_ref.shape[0], chunk):
        acc = base_ref[start:start + size, :].astype(F32)
        for x_ref, w_ref in zip(xs, ws):
            acc = acc + jnp.dot(x_ref[start:start + size, :], w_ref[...], preferred_element_type=F32)
        if b_ref is not None:
            acc = acc + b_ref[...]
        o_ref[start:start + size, :] = acc.astype(o_ref.dtype)


def add_products(terms, base, bias, out_dtype, bm, bn, chunk=256):
    rows, cols = base.shape
    k = terms[0][2].shape[0]
    n_terms = len(terms)
    kernel = functools.partial(sum_kernel, n_terms, chunk)
    specs = [pl.BlockSpec((bm, k), functools.partial(lambda o, m, n: (m, o), xc // k)) for _, xc, _, _ in terms]
    specs += [pl.BlockSpec((k, bn), functools.partial(lambda o, m, n: (0, n + o), wc // bn)) for _, _, _, wc in terms]
    specs.append(pl.BlockSpec((bm, bn), lambda m, n: (m, n)))
    args = [t[0] for t in terms] + [t[2] for t in terms] + [base]
    if bias is not None:
        specs.append(pl.BlockSpec((1, bn), lambda m, n: (0, n)))
        args.append(bias)
        body = kernel
    else:
        def body(*refs):
            kernel(*refs[:-1], None, refs[-1])
    return pl.pallas_call(
        body,
        out_shape=jax.ShapeDtypeStruct((rows, cols), out_dtype),
        grid=(rows // bm, cols // bn),
        in_specs=specs,
        out_specs=pl.BlockSpec((bm, bn), lambda m, n: (m, n)),
        compiler_params=params(58, 2),
        cost_estimate=cost(2 * n_terms * rows * k * cols, 2 * n_terms * (rows * k + k * cols) + 6 * rows * cols),
    )(*args)


def solution(mesh):
    batch_axes = ('dp', 'fsdp')
    n_dev = mesh.shape['fsdp']

    def gather_full(shard):
        return lax.all_gather(shard, 'fsdp', axis=0, tiled=True)

    def local_layer(prompts, ln1_gain, ln1_bias, w_qkv, b_qkv, w_out, b_out, ln2_gain, ln2_bias, w_up, b_up, w_down, b_down):
        batch, seq, d = prompts.shape
        heads, head_dim = w_qkv.shape[2], w_qkv.shape[3]
        width = heads * head_dim
        own = w_out.shape[0]
        n_slabs = w_up.shape[1] // d
        rows = batch * seq

        small = jnp.concatenate(
            [v.reshape(-1, own) for v in (ln1_gain, ln1_bias, b_out, ln2_gain, ln2_bias, b_down, b_qkv, b_up)], axis=0)
        n_small = small.shape[0]
        small = jnp.pad(small, ((0, -n_small % 16), (0, -own % LANES)))
        up_slabs = w_up.reshape(own, n_dev, n_slabs, own).transpose(0, 2, 1, 3).reshape(own, n_slabs * d)
        down_slabs = [w_down[u * own:(u + 1) * own] for u in range(n_slabs)]

        cut = (n_slabs - 1) * d
        full_a = gather_full(w_qkv.reshape(own, 3 * width))
        vectors = lax.all_gather(small, 'fsdp', axis=0, tiled=False)[:, :n_small, :own].astype(F32)
        full_b = gather_full(jnp.concatenate([w_out, up_slabs[:, :cut]], axis=1))
        full_c = gather_full(jnp.concatenate([up_slabs[:, cut:], down_slabs[0], down_slabs[1]], axis=1))
        full_d = gather_full(jnp.concatenate(down_slabs[2:], axis=1))

        bqkv = vectors[:, 6:9].reshape(1, 3 * width)
        vectors = vectors.transpose(1, 0, 2).reshape(n_small, d)
        g1, s1, bo, g2, s2, bd = [vectors[i:i + 1] for i in range(6)]
        bup = vectors[9:].reshape(1, n_slabs * d)

        x = prompts.reshape(rows, d)
        normed1 = norm_rows(x, g1, s1)
        gelu = functools.partial(jax.nn.gelu, approximate=True)
        q, k_t, v_t = queries_keys_values(normed1, full_a, width, bqkv, seq)
        ctx = attention(q, k_t, v_t, heads, head_dim)
        x1 = add_products([(ctx, 0, full_b, 0)], x, bo, BF16, rows, 256)
        normed2 = norm_rows(x1, g2, s2)
        hid_a = project(normed2, full_b, width, cut, bup[:, :cut], gelu, rows, 256)
        normed2, hid_a = lax.optimization_barrier((normed2, hid_a))
        hid_b = project(normed2, full_c, 0, d, bup[:, cut:], gelu, rows, 256)
        part = add_products([(hid_a, 0, full_c, d), (hid_a, d, full_c, 2 * d)], x1, bd, F32, rows // 2, 256)
        y = add_products([(hid_a, 2 * d, full_d, 0), (hid_b, 0, full_d, d)], part, None, BF16, rows // 2, 256)

        def cache(t):
            return t.reshape(batch, heads, head_dim, seq).transpose(0, 3, 1, 2)

        return y.reshape(batch, seq, d), cache(k_t), cache(v_t)

    weight_spec = P('fsdp')
    return jax.shard_map(local_layer, mesh=mesh, in_specs=(P(batch_axes),) + (weight_spec,) * 12, out_specs=(P(batch_axes), P(batch_axes), P(batch_axes)), check_vma=False)
```
